32 devices in a mesh: seq: 16 (over z, y, x), head: 2 (over core).
Axes of the slice: x: 2, y: 2, z: 4, core: 2. Of those that a mesh axis runs over, the one named last changes fastest.
Arguments:
- queries: bfloat16 [4096, 64, 192], P('seq', 'head'), may hold values from -50 to 50
- grad_out: bfloat16 [4096, 64, 128], P('seq', 'head'), may hold values from -6 to 6
- latent: bfloat16 [4096, 576], P('seq'), may hold values from -18 to 18
- w_uk: bfloat16 [64, 512, 128], P('head'), may hold values from -0.25 to 0.25
- w_uv: bfloat16 [64, 512, 128], P('head'), may hold values from -0.25 to 0.25
- doc_start: int32 [4096], P('seq'), may hold values from 0 to 4095, as said below
Outputs:
- grad_query: bfloat16 [4096, 64, 192], P('seq', 'head')
- grad_latent: float32 [4096, 576], P(('seq', 'head'))
The draws below stay inside these ranges and needn't reach their ends.
Inputs may be any that keep to these rules, and one draw needn't show every extreme that they name: doc_start[t] is the first position of the document that holds position t; documents follow one another, each of 1 to 768 positions, and one is exactly 768 long.
All inputs are finite; a program needn't handle non-finite values.
Results may differ from the reference program's by a relative error of at most 0.008.
Values may be sent and summed in bfloat16 or wider, within the bound.
A program may use at most 192 MiB of HBM per device.

```python
import jax
import jax.numpy as jnp
from jax import lax

HEADS = 64
NOPE = 128
ROPE = 64
LATENT = 512
VDIM = 128
T_DEV = 256
BACK = 3
MOST = 768
SEQ = 4096
N_SEQ = 16


def draw_latent(key, part):
    values = jnp.clip(jax.random.normal(jax.random.fold_in(key, 11), (SEQ, LATENT + ROPE), jnp.float32), -6.0, 6.0)
    return values.astype(jnp.bfloat16)


def draw_queries(key, part):
    values = jnp.clip(jax.random.normal(jax.random.fold_in(key, 21), (SEQ, HEADS, NOPE + ROPE), jnp.float32), -6.0, 6.0)
    return values.astype(jnp.bfloat16)


def draw_doc_start(key, part):
    key_len, key_first = jax.random.split(jax.random.fold_in(key, 31))
    lengths = jax.random.randint(key_len, (SEQ,), 1, MOST + 1)
    first = jax.random.randint(key_first, (), 1, T_DEV)
    lengths = lengths.at[0].set(first).at[1].set(MOST)
    ends = jnp.cumsum(lengths).astype(jnp.int32)
    starts = (ends - lengths).astype(jnp.int32)
    position = jnp.arange(SEQ, dtype=jnp.int32)
    which = jnp.searchsorted(ends, position, side='right')
    result = starts[which].astype(jnp.int32)
    result = jnp.where(position == SEQ - 1, SEQ - 1, result)
    return result.astype(jnp.int32)


def block_levels(own_key, shape, shards, least, top_value):
    factor_of = 1.0
    for dim, blocks in shards:
        draws = jax.random.uniform(jax.random.fold_in(jax.random.fold_in(own_key, 6), dim), (blocks,), jnp.float32, least / len(shards), top_value / len(shards))
        factor_of = factor_of * jnp.repeat(jnp.exp(draws), shape[dim] // blocks).reshape((-1,) + (1,) * (len(shape) - 1 - dim))
    return factor_of


def normal_values(stream_key, dims, scale, most, cuts=(), kind=jnp.bfloat16):
    drawn = jax.random.normal(stream_key, dims, jnp.float32) * scale
    if len(cuts) > 0:
        drawn = block_levels(stream_key, dims, cuts, -0.22, 0.18) * drawn
    return jnp.clip(drawn, min=-most, max=most).astype(kind)


def setup_inputs(seed: int = 0) -> dict:
    splits = jax.random.split(jax.random.key(seed), 7)
    queries = draw_queries(jax.random.fold_in(splits[6], 71), 0)
    grad_out = normal_values(splits[1], (SEQ, HEADS, VDIM), 1.0, 6.0, ((0, 16), (1, 2)))
    latent = draw_latent(jax.random.fold_in(splits[6], 71), 0)
    w_uk = normal_values(splits[3], (HEADS, LATENT, NOPE), LATENT ** -0.5, 0.25, ((0, 2),))
    w_uv = normal_values(splits[4], (HEADS, LATENT, VDIM), LATENT ** -0.5, 0.25, ((0, 2),))
    doc_start = draw_doc_start(jax.random.fold_in(splits[6], 71), 0)
    return dict(queries=queries, grad_out=grad_out, latent=latent, w_uk=w_uk, w_uv=w_uv, doc_start=doc_start)


def rounded(values):
    return lax.optimization_barrier(values.astype(jnp.bfloat16)).astype(jnp.float32)


def reference(queries, grad_out, latent, w_uk, w_uv, doc_start):
    width = LATENT + ROPE
    factor = (NOPE + ROPE) ** -0.5
    span = (BACK + 1) * T_DEV
    front = BACK * T_DEV
    padded = jnp.concatenate([jnp.zeros((front, width), latent.dtype), latent], 0)
    uk_full = w_uk.astype(jnp.float32)
    uv_full = w_uv.astype(jnp.float32)

    def step(carry, index):
        start = (index * T_DEV).astype(jnp.int32)
        query = lax.dynamic_slice_in_dim(queries, start, T_DEV, 0).astype(jnp.float32)
        cotangent = lax.dynamic_slice_in_dim(grad_out, start, T_DEV, 0).astype(jnp.float32)
        starts = lax.dynamic_slice_in_dim(doc_start, start, T_DEV, 0)
        keys = lax.dynamic_slice_in_dim(padded, start, span, 0).astype(jnp.float32)
        qpos = start + jnp.arange(T_DEV, dtype=jnp.int32)
        kpos = start - front + jnp.arange(span, dtype=jnp.int32)
        visible = (kpos[None, :] >= starts[:, None]) & (kpos[None, :] <= qpos[:, None])
        q_abs = rounded(jnp.einsum('thn,hln->thl', query[:, :, :NOPE], uk_full))
        qcat = jnp.concatenate([q_abs, query[:, :, NOPE:]], -1)
        scores = jnp.einsum('thc,uc->htu', qcat, keys) * factor
        scores = jnp.where(visible[None], scores, -jnp.inf)
        top = jnp.max(scores, -1, keepdims=True)
        expo = jnp.exp(scores - top)
        probs = rounded(expo / jnp.sum(expo, -1, keepdims=True))
        grad_lat = rounded(jnp.einsum('thv,hlv->thl', cotangent, uv_full))
        o_lat = jnp.einsum('htu,ul->thl', probs, keys[:, :LATENT])
        delta = jnp.sum(grad_lat * o_lat, -1)
        dprob = jnp.einsum('thl,ul->htu', grad_lat, keys[:, :LATENT])
        dscore = rounded(probs * (dprob - delta.T[:, :, None]))
        dq_cat = jnp.einsum('htu,uc->thc', dscore, keys) * factor
        dq_nope = jnp.einsum('thl,hln->thn', rounded(dq_cat[:, :, :LATENT]), uk_full)
        grad_query = jnp.concatenate([dq_nope, dq_cat[:, :, LATENT:]], -1).astype(jnp.bfloat16)
        dkey = jnp.einsum('htu,thc->uc', dscore, qcat) * factor
        dvalue = jnp.einsum('htu,thl->ul', probs, grad_lat)
        dkey = dkey + jnp.pad(dvalue, ((0, 0), (0, ROPE)))
        window = lax.dynamic_slice_in_dim(carry, start, span, 0) + dkey
        carry = lax.dynamic_update_slice_in_dim(carry, window, start, 0)
        return carry, grad_query

    init = jnp.zeros((front + N_SEQ * T_DEV, width), jnp.float32)
    total, pieces = lax.scan(step, init, jnp.arange(N_SEQ, dtype=jnp.int32))
    return pieces.reshape(N_SEQ * T_DEV, HEADS, NOPE + ROPE), total[front:]
```

```python
import functools
import math

import jax
import jax.numpy as jnp
from jax import lax
from jax.experimental import pallas as pl
from jax.experimental.pallas import tpu as pltpu
from jax.sharding import PartitionSpec as P

BACK = 3
LANES = 128
PAIR = 2
HIDDEN = -1e30
F32 = jnp.float32
BF16 = jnp.bfloat16
NN = (((1,), (0,)), ((), ()))
NT = (((1,), (1,)), ((), ()))


def dot(a, b, dims=NN):
    return lax.dot_general(a, b, dims, preferred_element_type=F32)


def kernel(tokens, nope, latw, factor, halves, counts, side, starts, q_ref, g_ref, uk_ref, uv_ref, kt_ref,
           gq_ref, *refs):
    *sums, k_ref, bias_ref, acc_ref, qc_ref, gl_ref, dqa_ref = refs
    step = pl.program_id(0)
    width, span = kt_ref.shape
    blocks = tokens // LANES

    @pl.when(step == 0)
    def _():
        acc_ref[...] = jnp.zeros_like(acc_ref)
        for j in range(span // LANES):
            part = pl.ds(j * LANES, LANES)
            k_ref[part, :] = kt_ref[:, part].T
            kpos = lax.broadcasted_iota(jnp.int32, (LANES, tokens), 0) + j * LANES
            qpos = lax.broadcasted_iota(jnp.int32, (LANES, tokens), 1) + (span - tokens)
            seen = (kpos >= starts[...]) & (kpos <= qpos)
            bias_ref[part, :] = jnp.where(seen, 0.0, HIDDEN)

    for i in range(PAIR):
        columns = pl.ds(i * LANES, LANES)
        q_abs = dot(uk_ref[i], q_ref[i, :nope, :]).astype(BF16)
        grad_lat = dot(uv_ref[i], g_ref[i], NT).astype(BF16)
        for b in range(blocks):
            here = slice(b * LANES, (b + 1) * LANES)
            qc_ref[b, :latw, columns] = q_abs[:, here]
            qc_ref[b, latw:, columns] = q_ref[i, nope:, here]
            gl_ref[b, :, columns] = grad_lat[:, here]

    def attend(b, count):
        end = span - (blocks - 1 - b) * LANES
        rows = slice(end - count * LANES, end)
        here = slice(b * LANES, (b + 1) * LANES)
        bias = bias_ref[rows, here]
        scores = dot(k_ref[rows, :], qc_ref[b]) + jnp.concatenate([bias] * PAIR, 1)
        dprob = dot(k_ref[rows, :latw], gl_ref[b])
        top = jnp.max(scores, 0, keepdims=True)
        expo = jnp.exp2((scores - top) * (factor * math.log2(math.e)))
        probs = (expo * (1.0 / jnp.sum(expo, 0, keepdims=True))).astype(BF16)
        wide = probs.astype(F32)
        delta = jnp.sum(wide * dprob, 0, keepdims=True)
        dscore = (wide * (dprob - delta)).astype(BF16)
        dvalue = dot(gl_ref[b], probs, NT) * (1.0 / factor)
        dq = dot(kt_ref[:, rows], dscore) * factor
        dkey = dot(qc_ref[b], dscore, NT)
        acc_ref[:latw, rows] += dkey[:latw] + dvalue
        acc_ref[latw:, rows] += dkey[latw:]
        for i in range(PAIR):
            columns = slice(i * LANES, (i + 1) * LANES)
            dqa_ref[i, :, here] = dq[:latw, columns].astype(BF16)
            gq_ref[i, nope:, here] = dq[latw:, columns].astype(BF16)

    most = span // LANES - blocks + 1
    sizes = sorted({2, 4, *range(5, most), most})
    for b in range(blocks):
        least = 0
        for size in sizes:
            count = counts[b]
            fits = (count > least) & (count <= size)
            pl.when(fits)(functools.partial(attend, b, size))
            least = size

    for i in range(PAIR):
        gq_ref[i, :nope, :] = dot(uk_ref[i].T, dqa_ref[i]).astype(BF16)

    @pl.when(step == pl.num_programs(0) - 1)
    def _():
        if not halves:
            for r in range(span // tokens):
                sums[0][r] = acc_ref[:, r * tokens:(r + 1) * tokens] * factor
            return
        mine_ref, theirs_ref = sums
        half = tokens // 2
        for r in range(span // tokens):
            own = pl.ds(pl.multiple_of(r * tokens + side[0] * half, half), half)
            other = pl.ds(pl.multiple_of(r * tokens + (1 - side[0]) * half, half), half)
            mine_ref[r] = acc_ref[:, own] * factor
            theirs_ref[r] = (acc_ref[:, other] * factor).astype(BF16)


def shift(block, axis, distance):
    devices = range(lax.axis_size(axis))
    route = [(i - distance, i) for i in devices if i - distance in devices]
    return lax.ppermute(block, axis, route)


def shards(queries, grad_out, latent, w_uk, w_uv, doc_start):
    tokens, heads, depth = queries.shape
    width = latent.shape[1]
    latw, nope = w_uk.shape[1:]
    vdim = w_uv.shape[2]
    span = (BACK + 1) * tokens
    blocks = tokens // LANES
    factor = depth ** (-0.5)
    own = latent.T
    received = [shift(own, "seq", level) for level in range(BACK, 0, -1)]
    keys = jnp.concatenate(received + [own], 1)
    starts = doc_start - (lax.axis_index("seq") - BACK) * tokens
    ends = (span - tokens) // LANES + 1 + jnp.arange(blocks, dtype=jnp.int32)
    counts = ends - starts[::LANES] // LANES
    side = lax.axis_index("head").astype(jnp.int32)[None]
    halves = lax.axis_size("head") == 2
    share = tokens // 2 if halves else tokens
    sums = [F32, BF16] if halves else [F32]

    def per_pair(*shape):
        return pl.BlockSpec((PAIR,) + shape, lambda p, *_: (p, 0, 0))

    def whole(*shape):
        return pl.BlockSpec(shape, lambda p, *_: (0,) * len(shape))

    grad_q, mine, *theirs = pl.pallas_call(
        functools.partial(kernel, tokens, nope, latw, factor, halves),
        grid_spec=pltpu.PrefetchScalarGridSpec(
            num_scalar_prefetch=2,
            grid=(heads // PAIR,),
            in_specs=[
                whole(1, tokens),
                per_pair(depth, tokens),
                per_pair(tokens, vdim),
                per_pair(latw, nope),
                per_pair(latw, vdim),
                whole(width, span),
            ],
            out_specs=[
                per_pair(depth, tokens),
                *[whole(BACK + 1, width, share) for _ in sums],
            ],
            scratch_shapes=[
                pltpu.VMEM((span, width), BF16),
                pltpu.VMEM((span, tokens), F32),
                pltpu.VMEM((width, span), F32),
                pltpu.VMEM((blocks, width, PAIR * LANES), BF16),
                pltpu.VMEM((blocks, latw, PAIR * LANES), BF16),
                pltpu.VMEM((PAIR, latw, tokens), BF16),
            ],
        ),
        out_shape=[
            jax.ShapeDtypeStruct((heads, depth, tokens), BF16),
            *[jax.ShapeDtypeStruct((BACK + 1, width, share), kind) for kind in sums],
        ],
        compiler_params=pltpu.CompilerParams(
            dimension_semantics=("arbitrary",), vmem_limit_bytes=60 * 1024 * 1024
        ),
        name="attend",
    )(
        counts,
        side,
        starts[None, :],
        queries.transpose(1, 2, 0),
        grad_out.transpose(1, 0, 2),
        w_uk,
        w_uv,
        keys,
    )
    grad_query = grad_q.transpose(2, 0, 1)
    summed = mine
    if halves:
        summed = mine + lax.ppermute(theirs[0], "head", [(0, 1), (1, 0)]).astype(F32)
    back = [shift(summed[BACK - r].astype(BF16), "seq", -r) for r in range(1, BACK + 1)]
    total = summed[BACK]
    for piece in back:
        total = total + piece.astype(F32)
    if not halves:
        return grad_query, lax.psum_scatter(total.T, "head", scatter_dimension=0, tiled=True)
    return grad_query, total.T


def solution(mesh):
    placed = (
        P("seq", "head", None),
        P("seq", "head", None),
        P("seq", None),
        P("head", None, None),
        P("head", None, None),
        P("seq"),
    )
    return jax.shard_map(
        shards,
        mesh=mesh,
        in_specs=placed,
        out_specs=(P("seq", "head", None), P(("seq", "head"), None)),
        check_vma=False,
    )
```

```python
import functools
import math

import jax
import jax.numpy as jnp
from jax import lax
from jax.experimental import pallas as pl
from jax.experimental.pallas import tpu as pltpu
from jax.sharding import PartitionSpec as P

BACK = 3
LANES = 128
PAIR = 2
GROUP = 2
HIDDEN = -1e30
F32 = jnp.float32
BF16 = jnp.bfloat16
NN = (((1,), (0,)), ((), ()))
NT = (((1,), (1,)), ((), ()))


def dot(a, b, dims=NN):
    return lax.dot_general(a, b, dims, preferred_element_type=F32)


def kernel(tokens, nope, latw, factor, halves, counts, side, starts, q_ref, g_ref, uk_ref, uv_ref, kt_ref,
           gq_ref, *refs):
    *sums, k_ref, bias_ref, acc_ref, qc_ref, gl_ref, dqa_ref = refs
    step = pl.program_id(0)
    width, span = kt_ref.shape
    blocks = tokens // LANES

    @pl.when(step == 0)
    def _():
        acc_ref[...] = jnp.zeros_like(acc_ref)
        for j in range(span // LANES):
            part = pl.ds(j * LANES, LANES)
            k_ref[part, :] = kt_ref[:, part].T
            kpos = lax.broadcasted_iota(jnp.int32, (LANES, tokens), 0) + j * LANES
            qpos = lax.broadcasted_iota(jnp.int32, (LANES, tokens), 1) + (span - tokens)
            seen = (kpos >= starts[...]) & (kpos <= qpos)
            bias_ref[part, :] = jnp.where(seen, 0.0, HIDDEN)

    def pair(index, carry):
        first = index * PAIR
        for i in range(PAIR):
            columns = pl.ds(i * LANES, LANES)
            q_abs = dot(uk_ref[first + i], q_ref[first + i, :nope, :]).astype(BF16)
            grad_lat = dot(uv_ref[first + i], g_ref[first + i], NT).astype(BF16)
            for b in range(blocks):
                here = slice(b * LANES, (b + 1) * LANES)
                qc_ref[b, :latw, columns] = q_abs[:, here]
                qc_ref[b, latw:, columns] = q_ref[first + i, nope:, here]
                gl_ref[b, :, columns] = grad_lat[:, here]

        def attend(b, count):
            end = span - (blocks - 1 - b) * LANES
            rows = slice(end - count * LANES, end)
            here = slice(b * LANES, (b + 1) * LANES)
            bias = bias_ref[rows, here]
            scores = dot(k_ref[rows, :], qc_ref[b]) + jnp.concatenate([bias] * PAIR, 1)
            dprob = dot(k_ref[rows, :latw], gl_ref[b])
            top = jnp.max(scores, 0, keepdims=True)
            expo = jnp.exp2((scores - top) * (factor * math.log2(math.e)))
            probs = (expo * (1.0 / jnp.sum(expo, 0, keepdims=True))).astype(BF16)
            wide = probs.astype(F32)
            delta = jnp.sum(wide * dprob, 0, keepdims=True)
            dscore = (wide * (dprob - delta)).astype(BF16)
            dvalue = dot(gl_ref[b], probs, NT) * (1.0 / factor)
            dq = dot(kt_ref[:, rows], dscore) * factor
            dkey = dot(qc_ref[b], dscore, NT)
            acc_ref[:latw, rows] += dkey[:latw] + dvalue
            acc_ref[latw:, rows] += dkey[latw:]
            for i in range(PAIR):
                columns = slice(i * LANES, (i + 1) * LANES)
                dqa_ref[i, :, here] = dq[:latw, columns].astype(BF16)
                gq_ref[first + i, nope:, here] = dq[latw:, columns].astype(BF16)

        most = span // LANES - blocks + 1
        sizes = sorted({2, 4, *range(5, most), most})
        for b in range(blocks):
            least = 0
            for size in sizes:
                count = counts[b]
                fits = (count > least) & (count <= size)
                pl.when(fits)(functools.partial(attend, b, size))
                least = size

        for i in range(PAIR):
            gq_ref[first + i, :nope, :] = dot(uk_ref[first + i].T, dqa_ref[i]).astype(BF16)
        return carry

    lax.fori_loop(0, q_ref.shape[0] // PAIR, pair, 0)

    @pl.when(step == pl.num_programs(0) - 1)
    def _():
        if not halves:
            for r in range(span // tokens):
                sums[0][r] = acc_ref[:, r * tokens:(r + 1) * tokens] * factor
            return
        mine_ref, theirs_ref = sums
        half = tokens // 2
        for r in range(span // tokens):
            own = pl.ds(pl.multiple_of(r * tokens + side[0] * half, half), half)
            other = pl.ds(pl.multiple_of(r * tokens + (1 - side[0]) * half, half), half)
            mine_ref[r] = acc_ref[:, own] * factor
            theirs_ref[r] = (acc_ref[:, other] * factor).astype(BF16)


def places():
    me = lax.axis_index("seq")
    count = lax.axis_size("seq")
    head = lax.axis_index("head")
    ahead = [(lax.rem(me + r, count), head) for r in range(1, BACK + 1)]
    behind = [(lax.rem(me + count - r, count), head) for r in range(1, BACK + 1)]
    return head, ahead, behind, (me, 1 - head)


def meet(peers):
    barrier = pltpu.get_barrier_semaphore()
    for peer in peers:
        pl.semaphore_signal(barrier, inc=1, device_id=peer, device_id_type=pl.DeviceIdType.MESH)
    pl.semaphore_wait(barrier, len(peers))


def send(src, dst, sems, slot, peer):
    copy = pltpu.make_async_remote_copy(
        src_ref=src, dst_ref=dst, send_sem=sems.at[0, slot], recv_sem=sems.at[1, slot],
        device_id=peer, device_id_type=pl.DeviceIdType.MESH,
    )
    copy.start()
    return copy


def gather_kernel(own_ref, keys_ref, far_sems, near_sems):
    tokens = own_ref.shape[1]
    half = tokens // 2
    head, ahead, behind, sibling = places()
    meet(ahead + behind + [sibling])
    mine = pl.ds(pl.multiple_of(head * half, half), half)
    landing = [
        keys_ref.at[:, pl.ds(pl.multiple_of((BACK - r) * tokens + head * half, half), half)]
        for r in range(1, BACK + 1)
    ]
    far = [send(own_ref.at[:, mine], landing[r], far_sems, r, ahead[r]) for r in range(BACK)]
    keys_ref[:, BACK * tokens:] = own_ref[...]
    near = []
    for r in range(BACK):
        far[r].wait_recv()
        near.append(send(landing[r], landing[r], near_sems, r, sibling))
    for r in range(BACK):
        far[r].wait_send()
        near[r].wait()


def gather(own):
    width, tokens = own.shape
    return pl.pallas_call(
        gather_kernel,
        out_shape=jax.ShapeDtypeStruct((width, (BACK + 1) * tokens), own.dtype),
        in_specs=[pl.BlockSpec(memory_space=pltpu.VMEM)],
        out_specs=pl.BlockSpec(memory_space=pltpu.VMEM),
        scratch_shapes=[pltpu.SemaphoreType.DMA((2, BACK)), pltpu.SemaphoreType.DMA((2, BACK))],
        compiler_params=pltpu.CompilerParams(collective_id=0, has_side_effects=True),
        name="gather",
    )(own)


def combine_kernel(mine_ref, theirs_ref, out_ref, near_ref, part_ref, far_ref, near_sems, far_sems):
    _, ahead, behind, sibling = places()
    meet(ahead + behind + [sibling])
    near = [
        send(theirs_ref.at[r], near_ref.at[r], near_sems, r, sibling) for r in range(BACK + 1)
    ]
    far = []
    for r in range(BACK):
        near[r].wait_recv()
        part_ref[r] = (mine_ref[r] + near_ref[r].astype(F32)).astype(BF16)
        far.append(send(part_ref.at[r], far_ref.at[r], far_sems, r, behind[BACK - 1 - r]))
    near[BACK].wait_recv()
    out_ref[...] = mine_ref[BACK] + near_ref[BACK].astype(F32)
    for r in range(BACK):
        far[r].wait_recv()
        out_ref[...] += far_ref[r].astype(F32)
    for r in range(BACK + 1):
        near[r].wait_send()
    for r in range(BACK):
        far[r].wait_send()


def combine(mine, theirs):
    shape = mine.shape[1:]
    return pl.pallas_call(
        combine_kernel,
        out_shape=jax.ShapeDtypeStruct(shape, F32),
        in_specs=[pl.BlockSpec(memory_space=pltpu.VMEM)] * 2,
        out_specs=pl.BlockSpec(memory_space=pltpu.VMEM),
        scratch_shapes=[
            pltpu.VMEM((BACK + 1,) + shape, BF16),
            pltpu.VMEM((BACK,) + shape, BF16),
            pltpu.VMEM((BACK,) + shape, BF16),
            pltpu.SemaphoreType.DMA((2, BACK + 1)),
            pltpu.SemaphoreType.DMA((2, BACK)),
        ],
        compiler_params=pltpu.CompilerParams(collective_id=1, has_side_effects=True),
        name="combine",
    )(mine, theirs)


def shift(block, axis, distance):
    devices = range(lax.axis_size(axis))
    route = [(i - distance, i) for i in devices if i - distance in devices]
    return lax.ppermute(block, axis, route)


def shards(queries, grad_out, latent, w_uk, w_uv, doc_start):
    tokens, heads, depth = queries.shape
    width = latent.shape[1]
    latw, nope = w_uk.shape[1:]
    vdim = w_uv.shape[2]
    span = (BACK + 1) * tokens
    blocks = tokens // LANES
    factor = depth ** (-0.5)
    own = latent.T
    halves = lax.axis_size("head") == 2
    if halves:
        keys = gather(own)
    else:
        received = [shift(own, "seq", level) for level in range(BACK, 0, -1)]
        keys = jnp.concatenate(received + [own], 1)
    starts = doc_start - (lax.axis_index("seq") - BACK) * tokens
    ends = (span - tokens) // LANES + 1 + jnp.arange(blocks, dtype=jnp.int32)
    counts = ends - starts[::LANES] // LANES
    side = lax.axis_index("head").astype(jnp.int32)[None]
    share = tokens // 2 if halves else tokens
    sums = [F32, BF16] if halves else [F32]

    def per_pair(*shape):
        return pl.BlockSpec((PAIR * GROUP,) + shape, lambda p, *_: (p, 0, 0))

    def whole(*shape):
        return pl.BlockSpec(shape, lambda p, *_: (0,) * len(shape))

    grad_q, mine, *theirs = pl.pallas_call(
        functools.partial(kernel, tokens, nope, latw, factor, halves),
        grid_spec=pltpu.PrefetchScalarGridSpec(
            num_scalar_prefetch=2,
            grid=(heads // (PAIR * GROUP),),
            in_specs=[
                whole(1, tokens),
                per_pair(depth, tokens),
                per_pair(tokens, vdim),
                per_pair(latw, nope),
                per_pair(latw, vdim),
                whole(width, span),
            ],
            out_specs=[
                per_pair(depth, tokens),
                *[whole(BACK + 1, width, share) for _ in sums],
            ],
            scratch_shapes=[
                pltpu.VMEM((span, width), BF16),
                pltpu.VMEM((span, tokens), F32),
                pltpu.VMEM((width, span), F32),
                pltpu.VMEM((blocks, width, PAIR * LANES), BF16),
                pltpu.VMEM((blocks, latw, PAIR * LANES), BF16),
                pltpu.VMEM((PAIR, latw, tokens), BF16),
            ],
        ),
        out_shape=[
            jax.ShapeDtypeStruct((heads, depth, tokens), BF16),
            *[jax.ShapeDtypeStruct((BACK + 1, width, share), kind) for kind in sums],
        ],
        compiler_params=pltpu.CompilerParams(
            dimension_semantics=("arbitrary",), vmem_limit_bytes=60 * 1024 * 1024
        ),
        name="attend",
    )(
        counts,
        side,
        starts[None, :],
        queries.transpose(1, 2, 0),
        grad_out.transpose(1, 0, 2),
        w_uk,
        w_uv,
        keys,
    )
    grad_query = grad_q.transpose(2, 0, 1)
    if halves:
        return grad_query, combine(mine, theirs[0]).T
    back = [shift(mine[BACK - r].astype(BF16), "seq", -r) for r in range(1, BACK + 1)]
    total = mine[BACK]
    for piece in back:
        total = total + piece.astype(F32)
    return grad_query, lax.psum_scatter(total.T, "head", scatter_dimension=0, tiled=True)


def solution(mesh):
    placed = (
        P("seq", "head", None),
        P("seq", "head", None),
        P("seq", None),
        P("head", None, None),
        P("head", None, None),
        P("seq"),
    )
    return jax.shard_map(
        shards,
        mesh=mesh,
        in_specs=placed,
        out_specs=(P("seq", "head", None), P(("seq", "head"), None)),
        check_vma=False,
    )
```
